32 devices in a mesh: dp: 2 (over x), tp: 16 (over y, z, core).
Axes of the slice: x: 2, y: 2, z: 4, core: 2. Of those that a mesh axis runs over, the one named last changes fastest.
Arguments:
- x: bfloat16 [7168, 5120], P(('dp', 'tp')), parts along dimension 0
- w_gate: bfloat16 [5120, 32768], P(None, 'tp')
- w_up: bfloat16 [5120, 32768], P(None, 'tp')
- w_down: bfloat16 [32768, 5120], P('tp')
Outputs:
- output: bfloat16 [7168, 5120], P(('dp', 'tp')), parts along dimension 0
There are 2 independent parts. The reference program is written for one: setup_inputs(seed, part) draws one part's arguments, and reference() takes and returns one part's arrays. A program takes and returns all parts, laid end to end along the dimension named above; an argument that names none is the same for every part.
All inputs are finite; a program needn't handle non-finite values.
Results may differ from the reference program's by a relative error of at most 0.016.
Values are sent between devices in bfloat16 or wider.
A program may use at most 2 GiB of HBM per device.

```python
import jax
import jax.numpy as jnp

ROWS = 3584
D = 5120
FF = 32768


def setup_inputs(seed: int = 0, part: int = 0) -> dict:
    kx, kg, ku, kd = jax.random.split(jax.random.key(seed), 4)
    drawn = {
        "x": jax.random.normal(jax.random.fold_in(kx, part), (ROWS, D), jnp.float32),
        "w_gate": jax.random.normal(kg, (D, FF), jnp.float32) * D**-0.5,
        "w_up": jax.random.normal(ku, (D, FF), jnp.float32) * D**-0.5,
        "w_down": jax.random.normal(kd, (FF, D), jnp.float32) * FF**-0.5,
    }
    return {k: v.astype(jnp.bfloat16) for k, v in drawn.items()}


def reference(x, w_gate, w_up, w_down):
    gate = jnp.dot(x, w_gate, preferred_element_type=jnp.float32)
    up = jnp.dot(x, w_up, preferred_element_type=jnp.float32)
    hidden = (jax.nn.silu(gate) * up).astype(jnp.bfloat16)
    return jnp.dot(hidden, w_down, preferred_element_type=jnp.float32).astype(jnp.bfloat16)
```

```python
import jax
import jax.numpy as jnp
from jax import lax
from jax.experimental import pallas as pl
from jax.experimental.pallas import tpu as pltpu
from jax.sharding import PartitionSpec as P

MESH = pl.DeviceIdType.MESH
TILE = 512


def _device(r, c):
    y = r // 4
    z = r + y * (7 - 2 * r)
    return (y * 4 + z) * 2 + c


def _mlp_kernel(
    x, wg_hbm, wu_hbm, wd_hbm,
    out, xg, hid, parts, sums,
    wg, wu, xbuf, wd, hbuf, term, other, pin, rin,
    ag_send, ag_recv, dd_send, dd_recv, rs_send, rs_recv, pt_send, pt_recv,
    w_sem, x_sem, h_sem, hl_sem, wd_sem, in_sem, y_sem,
):
    half = x.shape[0] // 2
    d, ff = wg.shape
    ftiles = ff // TILE
    dtiles = d // TILE
    t = lax.axis_index("tp")
    c = t % 2
    z = (t // 2) % 4
    y = t // 8
    r = z + y * (7 - 2 * z)
    right = _device((r + 1) % 8, c)
    left = _device((r + 7) % 8, c)
    partner = t + 1 - 2 * c
    ring = (right, left)

    def rows(j, h, rel, n=1):
        return pl.ds(pl.multiple_of(((j * 2 + h) * 2 + rel) * half, half), n * half)

    def remote(src, dst, s, q, i, dev):
        return pltpu.make_async_remote_copy(
            src_ref=src, dst_ref=dst, send_sem=s.at[i], recv_sem=q.at[i],
            device_id={"tp": dev}, device_id_type=MESH,
        )

    def gathered(i, way):
        if way == 0:
            return (i + 1) // 2, (i + 1) % 2
        return (8 - (i + 1) // 2) % 8, 1 - (i + 1) % 2

    def ag_copy(m, way, own=False):
        h = m % 2 if way == 0 else 1 - m % 2
        j, jn = gathered(m + 1, way)[0], None
        src_j = m // 2 if way == 0 else (8 - m // 2) % 8
        src = x.at[pl.ds(h * half, half)] if own else xg.at[rows(src_j, h, 0)]
        return remote(src, xg.at[rows(j, h, 0)], ag_send, ag_recv, way * 7 + m, ring[way])

    def dd_copy(i, way, own=False):
        j, h = gathered(i, way)
        src = x.at[pl.ds(h * half, half)] if own else xg.at[rows(j, h, 0)]
        return remote(src, xg.at[rows(j, h, 1)], dd_send, dd_recv, way * 8 + i, partner)

    def w_copy(k, n):
        cols = pl.ds(pl.multiple_of(n * TILE, TILE), TILE)
        return pltpu.make_async_copy(
            (wg_hbm, wu_hbm)[k].at[:, cols], (wg, wu)[k].at[:, cols], w_sem.at[k, n]
        )

    def x_load(i, way):
        j, h = gathered(i, way)
        return pltpu.make_async_copy(
            xg.at[rows(j, h, 0, 2)], xbuf.at[pl.ds(way * 2 * half, 2 * half)], x_sem.at[way]
        )

    def h_store(i, way):
        j, h = gathered(i, way)
        return pltpu.make_async_copy(hbuf.at[way], hid.at[rows(j, h, 0, 2)], h_sem.at[way])

    barrier = pltpu.get_barrier_semaphore()
    for dev in (right, left, partner):
        pl.semaphore_signal(barrier, inc=1, device_id={"tp": dev}, device_id_type=MESH)
    pl.semaphore_wait(barrier, 3)

    for m in range(2):
        for way in range(2):
            ag_copy(m, way, own=True).start()
    for way in range(2):
        dd_copy(0, way, own=True).start()
    bounce = pltpu.make_async_copy(x, xbuf.at[pl.ds(2 * half, 2 * half)], x_sem.at[0])
    bounce.start()
    for n in range(ftiles):
        for k in range(2):
            w_copy(k, n).start()
    bounce.wait()
    for h in range(2):
        pltpu.make_async_copy(
            xbuf.at[pl.ds((2 + h) * half, half)], xg.at[rows(0, h, 0)], x_sem.at[h]
        ).start()
    for h in range(2):
        pltpu.make_async_copy(
            xbuf.at[pl.ds((2 + h) * half, half)], xg.at[rows(0, h, 0)], x_sem.at[h]
        ).wait()
    for way in range(2):
        dd_copy(0, way, own=True).wait_recv()
    x_load(0, 0).start()

    def stage(i, _):
        def tile(way, n):
            @pl.when((i == 0) & (way == 0))
            def _():
                for k in range(2):
                    w_copy(k, n).wait()

            cols = pl.ds(pl.multiple_of(n * TILE, TILE), TILE)
            block = xbuf[pl.ds(pl.multiple_of(way * 2 * half, 2 * half), 2 * half), :]
            gate = jnp.dot(block, wg[:, cols], preferred_element_type=jnp.float32)
            up = jnp.dot(block, wu[:, cols], preferred_element_type=jnp.float32)
            hbuf[way, :, cols] = (jax.nn.silu(gate) * up).astype(jnp.bfloat16)

        def work(s, _):
            way, n = s // ftiles, s % ftiles

            @pl.when(s == 0)
            def _():
                x_load(i, 0).wait()
                x_load(i, 1).start()

                @pl.when(i > 0)
                def _():
                    h_store(i - 1, 0).wait()

            @pl.when(s == ftiles)
            def _():
                h_store(i, 0).start()
                x_load(i, 1).wait()

                @pl.when(i > 0)
                def _():
                    h_store(i - 1, 1).wait()

            @pl.when((s == 2 * ftiles - 1) & (i < 7))
            def _():
                for w in range(2):
                    ag_copy(i, w).wait_recv()

                    @pl.when(i < 5)
                    def _():
                        ag_copy(i + 2, w).start()

                    dd_copy(i + 1, w).start()

            tile(way, n)
            return 0

        lax.fori_loop(0, 2 * ftiles, work, 0)
        h_store(i, 1).start()

        @pl.when(i < 7)
        def _():
            for w in range(2):
                dd_copy(i + 1, w).wait_recv()
            x_load(i + 1, 0).start()

        return 0

    lax.fori_loop(0, 8, stage, 0)
    for way in range(2):
        h_store(7, way).wait()

    def drain(m, _):
        for way in range(2):
            ag_copy(m, way).wait_send()
        return 0

    lax.fori_loop(0, 7, drain, 0)

    def drain_pair(i, _):
        for way in range(2):
            dd_copy(i, way).wait_send()
        return 0

    lax.fori_loop(0, 8, drain_pair, 0)

    def target(q):
        m, way = q // 2, q % 2
        sign = 1 - 2 * way
        j = (12 + sign * ((m + 1) // 2)) % 8
        h = way + sign * (m % 2)
        return j, h

    def h_load(q):
        j, h = target(q)
        return pltpu.make_async_copy(hid.at[rows(j, h, 0, 2)], hbuf.at[q % 2], hl_sem.at[q % 2])

    def wd_copy(g):
        n = g % dtiles
        cols = pl.ds(pl.multiple_of(n * TILE, TILE), TILE)
        return pltpu.make_async_copy(wd_hbm.at[:, cols], wd.at[g % 2], wd_sem.at[g % 2])

    def slot(ref, i):
        return ref.at[pl.ds(pl.multiple_of(i * half, half), half)]

    def pt_copy(q):
        return remote(other.at[q % 2], slot(parts, q), pt_send, pt_recv, q, partner)

    def rs_copy(m, way):
        i = way * 7 + m
        return remote(slot(xbuf, way * 2 + m % 2), slot(sums, i), rs_send, rs_recv, i, ring[way])

    h_load(0).start()
    wd_copy(0).start()

    def down(q):
        h_load(q).wait()

        @pl.when(q < 15)
        def _():
            h_load(q + 1).start()

        @pl.when(q >= 2)
        def _():
            pt_copy(q - 2).wait_send()

        def tile(n, _):
            g = q * dtiles + n
            wd_copy(g).wait()

            @pl.when(g + 1 < 16 * dtiles)
            def _():
                wd_copy(g + 1).start()

            cols = pl.ds(pl.multiple_of(n * TILE, TILE), TILE)
            prod = jnp.dot(hbuf[q % 2], wd[g % 2], preferred_element_type=jnp.float32)
            term[q % 2, :, cols] = prod[:half]
            other[q % 2, :, cols] = prod[half:].astype(jnp.bfloat16)
            return 0

        lax.fori_loop(0, dtiles, tile, 0)
        pt_copy(q).start()

    def fetch(src, dst, i):
        return pltpu.make_async_copy(src, dst, in_sem.at[i])

    def add(q, to, sources):
        def tile(n, _):
            cols = pl.ds(pl.multiple_of(n * TILE, TILE), TILE)
            total = term[q % 2, :, cols] + pin[:, cols].astype(jnp.float32)
            for s in range(sources):
                total += rin[s, :, cols].astype(jnp.float32)
            to[:, cols] = total.astype(jnp.bfloat16)
            return 0

        lax.fori_loop(0, dtiles, tile, 0)

    def send(q, way):
        m = q // 2
        pt_copy(q).wait_recv()
        own = fetch(slot(parts, q), pin, 0)
        own.start()

        @pl.when(m >= 2)
        def _():
            rs_copy(m - 2, way).wait_recv()
            got = fetch(slot(sums, way * 7 + m - 2), rin.at[0], 1)
            got.start()
            rs_copy(m - 2, way).wait_send()
            got.wait()

        own.wait()
        to = slot(xbuf, way * 2 + m % 2)

        @pl.when(m >= 2)
        def _():
            add(q, to, 1)

        @pl.when(m < 2)
        def _():
            add(q, to, 0)

        rs_copy(m, way).start()

    def finish(q):
        way = q - 14
        h = 1 - way
        pt_copy(q).wait_recv()
        own = fetch(slot(parts, q), pin, 0)
        own.start()
        last = ((5, 6), (6, 5))[way]
        for w in range(2):
            rs_copy(last[w], w).wait_recv()
            fetch(slot(sums, w * 7 + last[w]), rin.at[w], 1 + w).start()
        for w in range(2):
            fetch(slot(sums, w * 7 + last[w]), rin.at[w], 1 + w).wait()
        own.wait()
        add(q, other.at[way], 2)
        pltpu.make_async_copy(other.at[way], out.at[pl.ds(h * half, half)], y_sem.at[way]).start()

    down(0)

    def step(q, _):
        @pl.when(q < 16)
        def _():
            down(q)

        for way in range(2):
            @pl.when((q - 1) % 2 == way)
            def _():
                send(q - 1, way)
        return 0

    lax.fori_loop(1, 15, step, 0)
    down(15)
    pt_copy(14).wait_send()
    finish(14)
    pt_copy(15).wait_send()
    finish(15)
    for way in range(2):
        pltpu.make_async_copy(
            other.at[way], out.at[pl.ds((1 - way) * half, half)], y_sem.at[way]
        ).wait()
        for m in (5, 6):
            rs_copy(m, way).wait_send()


def solution(mesh):
    def step(x, w_gate, w_up, w_down):
        n, d = x.shape
        ff = w_gate.shape[1]
        half = n // 2
        bf = jnp.bfloat16
        hbm = pl.BlockSpec(memory_space=pl.ANY)
        dma = pltpu.SemaphoreType.DMA
        result = pl.pallas_call(
            _mlp_kernel,
            out_shape=[
                jax.ShapeDtypeStruct((n, d), bf),
                jax.ShapeDtypeStruct((16 * n, d), bf),
                jax.ShapeDtypeStruct((16 * n, ff), bf),
                jax.ShapeDtypeStruct((16 * half, d), bf),
                jax.ShapeDtypeStruct((14 * half, d), bf),
            ],
            in_specs=[hbm] * 4,
            out_specs=[hbm] * 5,
            scratch_shapes=[
                pltpu.VMEM((d, ff), bf),
                pltpu.VMEM((d, ff), bf),
                pltpu.VMEM((4 * half, d), bf),
                pltpu.VMEM((2, ff, TILE), bf),
                pltpu.VMEM((2, n, ff), bf),
                pltpu.VMEM((2, half, d), jnp.float32),
                pltpu.VMEM((2, half, d), bf),
                pltpu.VMEM((half, d), bf),
                pltpu.VMEM((2, half, d), bf),
                dma((14,)), dma((14,)), dma((16,)), dma((16,)),
                dma((14,)), dma((14,)), dma((16,)), dma((16,)),
                dma((2, ff // TILE)), dma((2,)), dma((2,)), dma((2,)), dma((2,)), dma((3,)), dma((2,)),
            ],
            compiler_params=pltpu.CompilerParams(
                collective_id=0, has_side_effects=True, vmem_limit_bytes=67043328
            ),
        )(x, w_gate, w_up, w_down)
        return result[0]

    return jax.shard_map(
        step,
        mesh=mesh,
        in_specs=(P(("dp", "tp"), None), P(None, "tp"), P(None, "tp"), P("tp", None)),
        out_specs=P(("dp", "tp"), None),
        check_vma=False,
    )
```

```python
import jax
import jax.numpy as jnp
from jax import lax
from jax.experimental import pallas as pl
from jax.experimental.pallas import tpu as pltpu
from jax.sharding import PartitionSpec as P

MESH = pl.DeviceIdType.MESH
TILE = 512
EARLY = 256


def _device(r, c):
    y = r // 4
    z = r + y * (7 - 2 * r)
    return (y * 4 + z) * 2 + c


def _mlp_kernel(
    x, wg_hbm, wu_hbm, wd_hbm,
    out, xg, hid, parts, sums,
    w, xbuf, wd, hbuf, term, other, pin, rin,
    ag_send, ag_recv, dd_send, dd_recv, rs_send, rs_recv, pt_send, pt_recv,
    w_sem, x_sem, h_sem, wd_sem, early_sem, in_sem, y_sem,
):
    half = x.shape[0] // 2
    n_rows = 2 * half
    d, ff = wg_hbm.shape
    ftiles = ff // TILE
    dtiles = d // TILE
    wide = ff // 2
    t = lax.axis_index("tp")
    c = t % 2
    z = (t // 2) % 4
    y = t // 8
    r = z + y * (7 - 2 * z)
    right = _device((r + 1) % 8, c)
    left = _device((r + 7) % 8, c)
    partner = t + 1 - 2 * c
    ring = (right, left)

    def span(i, n, size):
        return pl.ds(pl.multiple_of(i * size, size), n * size)

    def rows(j, h, rel, n=1):
        return span((j * 2 + h) * 2 + rel, n, half)

    def remote(src, dst, s, q, i, dev):
        return pltpu.make_async_remote_copy(
            src_ref=src, dst_ref=dst, send_sem=s.at[i], recv_sem=q.at[i],
            device_id={"tp": dev}, device_id_type=MESH,
        )

    def gathered(i, way):
        if way == 0:
            return (i + 1) // 2, (i + 1) % 2
        return (8 - (i + 1) // 2) % 8, 1 - (i + 1) % 2

    def ag_copy(m, way, own=False):
        h = m % 2 if way == 0 else 1 - m % 2
        j = gathered(m + 1, way)[0]
        src_j = m // 2 if way == 0 else (8 - m // 2) % 8
        src = x.at[pl.ds(h * half, half)] if own else xg.at[rows(src_j, h, 0)]
        return remote(src, xg.at[rows(j, h, 0)], ag_send, ag_recv, way * 7 + m, ring[way])

    def dd_copy(i, way, own=False):
        j, h = gathered(i, way)
        src = x.at[pl.ds(h * half, half)] if own else xg.at[rows(j, h, 0)]
        return remote(src, xg.at[rows(j, h, 1)], dd_send, dd_recv, way * 8 + i, partner)

    def w_copy(k, n):
        cols = span(n, 1, TILE)
        return pltpu.make_async_copy(
            (wg_hbm, wu_hbm)[k].at[:, cols], w.at[pl.ds(k * d, d), cols], w_sem.at[k, n]
        )

    def x_load(i, way):
        j, h = gathered(i, way)
        return pltpu.make_async_copy(
            xg.at[rows(j, h, 0, 2)], xbuf.at[pl.ds(way * n_rows, n_rows)], x_sem.at[way]
        )

    def h_store(i, way):
        j, h = gathered(i, way)
        return pltpu.make_async_copy(
            hbuf.at[pl.ds(way * n_rows, n_rows)], hid.at[rows(j, h, 0, 2)], h_sem.at[way]
        )

    def slot(ref, i):
        return ref.at[span(i, 1, half)]

    def pt_copy(q):
        return remote(other.at[q % 2], slot(parts, q), pt_send, pt_recv, q, partner)

    def rs_copy(m, way, first=False):
        i = way * 7 + m
        src = rin.at[way] if first else slot(xbuf, way * 2 + m % 2)
        return remote(src, slot(sums, i), rs_send, rs_recv, i, ring[way])

    def fetch(src, dst, i):
        return pltpu.make_async_copy(src, dst, in_sem.at[i])

    def add(q, to, sources):
        def tile(n, _):
            cols = span(n, 1, TILE)
            total = term[q % 2, :, cols] + pin[:, cols].astype(jnp.float32)
            for s in range(sources):
                total += rin[s, :, cols].astype(jnp.float32)
            to[:, cols] = total.astype(jnp.bfloat16)
            return 0

        lax.fori_loop(0, dtiles, tile, 0)

    def early_copy(n):
        return pltpu.make_async_copy(
            wd_hbm.at[:, span(n, 1, EARLY)], wd.at[n % 4], early_sem.at[n % 4]
        )

    def early_terms():
        def tile(n, _):
            early_copy(n).wait()

            @pl.when(n + 3 < d // EARLY)
            def _():
                early_copy(n + 3).start()

            cols = span(n, 1, EARLY)
            prod = jnp.dot(hbuf[...], wd[n % 4], preferred_element_type=jnp.float32)
            term[1, :, cols] = prod[:half]
            other[1, :, cols] = prod[half:n_rows].astype(jnp.bfloat16)
            term[0, :, cols] = prod[n_rows : n_rows + half]
            other[0, :, cols] = prod[n_rows + half :].astype(jnp.bfloat16)
            return 0

        lax.fori_loop(0, d // EARLY, tile, 0)
        for q in range(2):
            pt_copy(q).start()

    def early_send():
        for q in range(2):
            pt_copy(q).wait_recv()
            own = fetch(slot(parts, q), pin, 0)
            own.start()
            own.wait()
            add(q, rin.at[q], 0)
            rs_copy(0, q, first=True).start()

    barrier = pltpu.get_barrier_semaphore()
    for dev in (right, left, partner):
        pl.semaphore_signal(barrier, inc=1, device_id={"tp": dev}, device_id_type=MESH)
    pl.semaphore_wait(barrier, 3)

    for m in range(2):
        for way in range(2):
            ag_copy(m, way, own=True).start()
    for way in range(2):
        dd_copy(0, way, own=True).start()
    bounce = pltpu.make_async_copy(x, xbuf.at[pl.ds(n_rows, n_rows)], x_sem.at[0])
    bounce.start()
    for n in range(ftiles):
        for k in range(2):
            w_copy(k, n).start()
    bounce.wait()
    stores = [
        pltpu.make_async_copy(
            xbuf.at[pl.ds((2 + h) * half, half)], xg.at[rows(0, h, 0)], x_sem.at[h]
        )
        for h in range(2)
    ]
    for s in stores:
        s.start()
    for s in stores:
        s.wait()
    for way in range(2):
        dd_copy(0, way, own=True).wait_recv()
    x_load(0, 0).start()

    def stage(i, _):
        @pl.when(i == 6)
        def _():
            early_terms()

        def work(s, _):
            way, n = (s // 2) % 2, s // 4 * 2 + s % 2

            for k in range(2):
                @pl.when(s == 2 * k)
                def _():
                    if k == 0:
                        x_load(i, 1).start()
                    x_load(i, k).wait()

                    @pl.when(i > 0)
                    def _():
                        h_store(i - 1, k).wait()

            @pl.when((s == 4) & (i == 6))
            def _():
                early_send()

            @pl.when((s == 4) & (i == 7))
            def _():
                for k in range(5):
                    wd_copy(k).start()

            @pl.when((s == 4) & (i == 5))
            def _():
                for k in range(3):
                    early_copy(k).start()

            @pl.when((s == 6) & (i < 7))
            def _():
                h_store(i, 0).start()

            @pl.when((s == 7) & (i < 7))
            def _():
                for k in range(2):
                    ag_copy(i, k).wait_recv()

                    @pl.when(i < 5)
                    def _():
                        ag_copy(i + 2, k).start()

                    dd_copy(i + 1, k).start()

            for k in range(2):
                @pl.when((i == 0) & (way == 0))
                def _():
                    w_copy(k, n).wait()

            cols = span(n, 1, TILE)
            block = xbuf[span(way, 1, n_rows), :]
            gate = jnp.dot(block, w[:d, cols], preferred_element_type=jnp.float32)
            up = jnp.dot(block, w[d:, cols], preferred_element_type=jnp.float32)
            hbuf[span(way, 1, n_rows), cols] = (jax.nn.silu(gate) * up).astype(jnp.bfloat16)
            return 0

        lax.fori_loop(0, 2 * ftiles, work, 0)

        @pl.when(i < 7)
        def _():
            h_store(i, 1).start()
            for k in range(2):
                dd_copy(i + 1, k).wait_recv()
            x_load(i + 1, 0).start()

        return 0

    def wd_copy(k):
        return pltpu.make_async_copy(
            wd_hbm.at[:, pl.ds(k * wide, wide)],
            w.at[pl.ds(k * ff, ff), pl.ds(0, wide)],
            wd_sem.at[k],
        )

    lax.fori_loop(0, 8, stage, 0)

    def target(q):
        m, way = q // 2, q % 2
        j = 4 + m // 2 + (1 - m % 2) - m // 6 + 2 * (m // 7)
        h = (1 - m % 2) * (1 - m // 6) + m // 7
        sign = 1 - 2 * way
        return (8 + sign * j) % 8, way + sign * h

    def h_load(q):
        j, h = target(q)
        return pltpu.make_async_copy(
            hid.at[rows(j, h, 0, 2)], hbuf.at[span(q % 2, 1, n_rows)], h_sem.at[q % 2]
        )

    def down(q):
        @pl.when(q >= 4)
        def _():
            h_load(q).wait()

        pt_copy(q - 2).wait_send()

        def tile(n, _):
            for k in range(5):
                @pl.when((q == 2) & (n == 2 * k))
                def _():
                    wd_copy(k).wait()

            block = w[span(n // 2, 1, ff), span(n % 2, 1, TILE)]
            prod = jnp.dot(
                hbuf[span(q % 2, 1, n_rows), :], block, preferred_element_type=jnp.float32
            )
            cols = span(n, 1, TILE)
            term[q % 2, :, cols] = prod[:half]
            other[q % 2, :, cols] = prod[half:].astype(jnp.bfloat16)
            return 0

        lax.fori_loop(0, dtiles, tile, 0)
        pt_copy(q).start()

        @pl.when(q < 14)
        def _():
            h_load(q + 2).start()

    def send(q, way):
        m = q // 2
        pt_copy(q).wait_recv()
        own = fetch(slot(parts, q), pin, 0)
        own.start()
        before = m - 2 + m // 6

        @pl.when(m >= 2)
        def _():
            rs_copy(before, way).wait_recv()
            rs_copy(m - 2, way).wait_send()
            got = fetch(slot(sums, way * 7 + before), rin.at[0], 1)
            got.start()
            got.wait()

        own.wait()
        to = slot(xbuf, way * 2 + m % 2)

        @pl.when(m >= 2)
        def _():
            add(q, to, 1)

        @pl.when(m < 2)
        def _():
            add(q, to, 0)

        rs_copy(m, way).start()

    def finish(q):
        way = q - 14
        h = 1 - way
        pt_copy(q).wait_recv()
        own = fetch(slot(parts, q), pin, 0)
        own.start()
        last = ((4, 6), (6, 4))[way]
        for k in range(2):
            rs_copy(last[k], k).wait_recv()
            fetch(slot(sums, k * 7 + last[k]), rin.at[k], 1 + k).start()
        for k in range(2):
            fetch(slot(sums, k * 7 + last[k]), rin.at[k], 1 + k).wait()
        own.wait()
        add(q, other.at[way], 2)
        pltpu.make_async_copy(other.at[way], out.at[pl.ds(h * half, half)], y_sem.at[way]).start()

    def step(q, _):
        down(q)
        for way in range(2):
            @pl.when((q > 2) & ((q - 1) % 2 == way))
            def _():
                send(q - 1, way)
        return 0

    lax.fori_loop(2, 15, step, 0)
    down(15)

    def drain(m, _):
        for way in range(2):
            ag_copy(m, way).wait_send()
        return 0

    def drain_pair(i, _):
        for way in range(2):
            dd_copy(i, way).wait_send()
        return 0

    lax.fori_loop(0, 7, drain, 0)
    lax.fori_loop(0, 8, drain_pair, 0)
    pt_copy(14).wait_send()
    finish(14)
    pt_copy(15).wait_send()
    finish(15)
    for way in range(2):
        pltpu.make_async_copy(
            other.at[way], out.at[pl.ds((1 - way) * half, half)], y_sem.at[way]
        ).wait()
        for m in (5, 6):
            rs_copy(m, way).wait_send()


def solution(mesh):
    def step(x, w_gate, w_up, w_down):
        n, d = x.shape
        ff = w_gate.shape[1]
        half = n // 2
        bf = jnp.bfloat16
        hbm = pl.BlockSpec(memory_space=pl.ANY)
        dma = pltpu.SemaphoreType.DMA
        result = pl.pallas_call(
            _mlp_kernel,
            out_shape=[
                jax.ShapeDtypeStruct((n, d), bf),
                jax.ShapeDtypeStruct((16 * n, d), bf),
                jax.ShapeDtypeStruct((16 * n, ff), bf),
                jax.ShapeDtypeStruct((16 * half, d), bf),
                jax.ShapeDtypeStruct((14 * half, d), bf),
            ],
            in_specs=[hbm] * 4,
            out_specs=[hbm] * 5,
            scratch_shapes=[
                pltpu.VMEM((2 * d, ff), bf),
                pltpu.VMEM((4 * half, d), bf),
                pltpu.VMEM((4, ff, EARLY), bf),
                pltpu.VMEM((2 * n, ff), bf),
                pltpu.VMEM((2, half, d), jnp.float32),
                pltpu.VMEM((2, half, d), bf),
                pltpu.VMEM((half, d), bf),
                pltpu.VMEM((2, half, d), bf),
                dma((14,)), dma((14,)), dma((16,)), dma((16,)),
                dma((14,)), dma((14,)), dma((16,)), dma((16,)),
                dma((2, ff // TILE)), dma((2,)), dma((2,)), dma((5,)), dma((4,)), dma((3,)), dma((2,)),
            ],
            compiler_params=pltpu.CompilerParams(
                collective_id=0, has_side_effects=True, vmem_limit_bytes=67043328
            ),
        )(x, w_gate, w_up, w_down)
        return result[0]

    return jax.shard_map(
        step,
        mesh=mesh,
        in_specs=(P(("dp", "tp"), None), P(None, "tp"), P(None, "tp"), P("tp", None)),
        out_specs=P(("dp", "tp"), None),
        check_vma=False,
    )
```

```python
import jax
import jax.numpy as jnp
from jax import lax
from jax.experimental import pallas as pl
from jax.experimental.pallas import tpu as pltpu
from jax.sharding import PartitionSpec as P

MESH = pl.DeviceIdType.MESH
TILE = 512
EARLY = 256
POLL_AT = 5
SEND_AT = 3


def _device(r, c):
    y = r // 4
    z = r + y * (7 - 2 * r)
    return (y * 4 + z) * 2 + c


def _mlp_kernel(
    x, wg_hbm, wu_hbm, wd_hbm,
    out, xg, hid, parts, sums,
    w, xbuf, wd, hbuf, term, other, pin, rin,
    ag_send, ag_recv, dd_send, dd_recv, rs_send, rs_recv, pt_send, pt_recv,
    w_sem, x_sem, h_sem, wd_sem, early_sem, in_sem, y_sem,
):
    half = x.shape[0] // 2
    n_rows = 2 * half
    d, ff = wg_hbm.shape
    ftiles = ff // TILE
    dtiles = d // TILE
    wide = ff // 2
    t = lax.axis_index("tp")
    c = t % 2
    z = (t // 2) % 4
    y = t // 8
    r = z + y * (7 - 2 * z)
    right = _device((r + 1) % 8, c)
    left = _device((r + 7) % 8, c)
    partner = t + 1 - 2 * c
    ring = (right, left)

    def span(i, n, size):
        return pl.ds(pl.multiple_of(i * size, size), n * size)

    def rows(j, h, rel, n=1):
        return span((j * 2 + h) * 2 + rel, n, half)

    def remote(src, dst, s, q, i, dev):
        return pltpu.make_async_remote_copy(
            src_ref=src, dst_ref=dst, send_sem=s.at[i], recv_sem=q.at[i],
            device_id={"tp": dev}, device_id_type=MESH,
        )

    def gathered(i, way):
        if way == 0:
            return (i + 1) // 2, (i + 1) % 2
        return (8 - (i + 1) // 2) % 8, 1 - (i + 1) % 2

    def ag_copy(m, way, own=False):
        h = m % 2 if way == 0 else 1 - m % 2
        j = gathered(m + 1, way)[0]
        src_j = m // 2 if way == 0 else (8 - m // 2) % 8
        src = x.at[pl.ds(h * half, half)] if own else xg.at[rows(src_j, h, 0)]
        return remote(src, xg.at[rows(j, h, 0)], ag_send, ag_recv, way * 7 + m, ring[way])

    def dd_copy(i, way, own=False):
        j, h = gathered(i, way)
        src = x.at[pl.ds(h * half, half)] if own else xg.at[rows(j, h, 0)]
        return remote(src, xg.at[rows(j, h, 1)], dd_send, dd_recv, way * 8 + i, partner)

    def w_copy(k, n):
        cols = span(n, 1, TILE)
        return pltpu.make_async_copy(
            (wg_hbm, wu_hbm)[k].at[:, cols], w.at[pl.ds(k * d, d), cols], w_sem.at[k, n]
        )

    def x_load(i, way):
        j, h = gathered(i, way)
        return pltpu.make_async_copy(
            xg.at[rows(j, h, 0, 2)], xbuf.at[pl.ds(way * n_rows, n_rows)], x_sem.at[way]
        )

    def h_store(i, way):
        j, h = gathered(i, way)
        return pltpu.make_async_copy(
            hbuf.at[pl.ds(way * n_rows, n_rows)], hid.at[rows(j, h, 0, 2)], h_sem.at[way]
        )

    def slot(ref, i):
        return ref.at[span(i, 1, half)]

    def pt_copy(q):
        return remote(other.at[q % 2], slot(parts, q), pt_send, pt_recv, q, partner)

    def rs_copy(m, way, first=False):
        i = way * 7 + m
        src = rin.at[way] if first else slot(xbuf, way * 2 + m % 2)
        return remote(src, slot(sums, i), rs_send, rs_recv, i, ring[way])

    def fetch(src, dst, i):
        return pltpu.make_async_copy(src, dst, in_sem.at[i])

    def add(q, to, sources, first=0, last=dtiles):
        def tile(n, _):
            cols = span(n, 1, TILE)
            total = term[q % 2, :, cols] + pin[:, cols].astype(jnp.float32)
            for s in range(sources):
                total += rin[s, :, cols].astype(jnp.float32)
            to[:, cols] = total.astype(jnp.bfloat16)
            return 0

        lax.fori_loop(first, last, tile, 0)

    def early_copy(n):
        return pltpu.make_async_copy(
            wd_hbm.at[:, span(n, 1, EARLY)], wd.at[n % 5], early_sem.at[n % 5]
        )

    def early_terms():
        def tile(n, _):
            early_copy(n).wait()

            @pl.when(n == d // EARLY - 4)
            def _():
                ready(6)

            @pl.when(n + 4 < d // EARLY)
            def _():
                early_copy(n + 4).start()

            cols = span(n, 1, EARLY)
            prod = jnp.dot(hbuf[...], wd[n % 5], preferred_element_type=jnp.float32)
            term[1, :, cols] = prod[:half]
            other[1, :, cols] = prod[half:n_rows].astype(jnp.bfloat16)
            term[0, :, cols] = prod[n_rows : n_rows + half]
            other[0, :, cols] = prod[n_rows + half :].astype(jnp.bfloat16)
            return 0

        lax.fori_loop(0, d // EARLY, tile, 0)
        for q in range(2):
            pt_copy(q).start()

    def early_send():
        for q in range(2):
            pt_copy(q).wait_recv()
            own = fetch(slot(parts, q), pin, 0)
            own.start()
            own.wait()
            add(q, rin.at[q], 0)
            rs_copy(0, q, first=True).start()

    barrier = pltpu.get_barrier_semaphore()
    for dev in (right, left, partner):
        pl.semaphore_signal(barrier, inc=1, device_id={"tp": dev}, device_id_type=MESH)
    pl.semaphore_wait(barrier, 3)

    for way in range(2):
        dd_copy(0, way, own=True).start()
    for m in range(2):
        for way in range(2):
            ag_copy(m, way, own=True).start()
    mine = [
        pltpu.make_async_copy(
            x.at[pl.ds((1 - way) * half, half)], xbuf.at[pl.ds(2 * way * half, half)], x_sem.at[way]
        )
        for way in range(2)
    ]
    theirs = [
        pltpu.make_async_copy(
            xg.at[rows(0, 1 - way, 1)], xbuf.at[pl.ds((2 * way + 1) * half, half)], h_sem.at[way]
        )
        for way in range(2)
    ]
    for way in range(2):
        mine[way].start()
    for n in range(ftiles):
        for k in range(2):
            w_copy(k, n).start()
    for way in range(2):
        dd_copy(0, way, own=True).wait_recv()
        theirs[way].start()
    for way in range(2):
        mine[way].wait()
        theirs[way].wait()

    def poll(m):
        for k in range(2):
            ag_copy(m, k).wait_recv()
            dd_copy(m + 1, k).start()

            @pl.when(m < 5)
            def _():
                ag_copy(m + 2, k).start()

    def ready(i):
        for k in range(2):
            dd_copy(i, k).wait_recv()
        x_load(i, 0).start()

    def stage(i, _):
        def work(s, _):
            way, n = (s // 2) % 2, s // 4 * 2 + s % 2

            for k in range(2):
                @pl.when(s == 2 * k)
                def _():
                    @pl.when(i > 0)
                    def _():
                        if k == 0:
                            x_load(i, 1).start()
                        x_load(i, k).wait()
                        h_store(i - 1, k).wait()

            @pl.when((s == SEND_AT) & (i == 6))
            def _():
                early_send()

            @pl.when((s == 4) & (i == 7))
            def _():
                for k in range(5):
                    wd_copy(k).start()

            @pl.when((s == 4) & (i == 5))
            def _():
                for k in range(4):
                    early_copy(k).start()

            @pl.when((s == 6) & (i < 7))
            def _():
                h_store(i, 0).start()

            @pl.when((s == POLL_AT) & (i < 7) & (i != 5))
            def _():
                poll(i)

            @pl.when((s == 7) & (i < 7) & (i != 5))
            def _():
                ready(i + 1)

            for k in range(2):
                @pl.when((i == 0) & (way == 0))
                def _():
                    w_copy(k, n).wait()

            cols = span(n, 1, TILE)
            block = xbuf[span(way, 1, n_rows), :]
            gate = jnp.dot(block, w[:d, cols], preferred_element_type=jnp.float32)
            up = jnp.dot(block, w[d:, cols], preferred_element_type=jnp.float32)
            hbuf[span(way, 1, n_rows), cols] = (jax.nn.silu(gate) * up).astype(jnp.bfloat16)
            return 0

        lax.fori_loop(0, 2 * ftiles, work, 0)

        @pl.when(i < 7)
        def _():
            h_store(i, 1).start()

        @pl.when(i == 5)
        def _():
            poll(5)
            early_terms()

        return 0

    def wd_copy(k):
        return pltpu.make_async_copy(
            wd_hbm.at[:, pl.ds(k * wide, wide)],
            w.at[pl.ds(k * ff, ff), pl.ds(0, wide)],
            wd_sem.at[k],
        )

    lax.fori_loop(0, 8, stage, 0)

    def target(q):
        m, way = q // 2, q % 2
        j = 4 + m // 2 + (1 - m % 2) - m // 6 + 2 * (m // 7)
        h = (1 - m % 2) * (1 - m // 6) + m // 7
        sign = 1 - 2 * way
        return (8 + sign * j) % 8, way + sign * h

    def h_load(q):
        j, h = target(q)
        return pltpu.make_async_copy(
            hid.at[rows(j, h, 0, 2)], hbuf.at[span(q % 2, 1, n_rows)], h_sem.at[q % 2]
        )

    def down(q):
        h_load(q).wait()

        @pl.when(q >= 6)
        def _():
            pt_copy(q - 2).wait_send()

        def tile(n, _):
            block = w[span(n // 2, 1, ff), span(n % 2, 1, TILE)]
            prod = jnp.dot(
                hbuf[span(q % 2, 1, n_rows), :], block, preferred_element_type=jnp.float32
            )
            cols = span(n, 1, TILE)
            term[q % 2, :, cols] = prod[:half]
            other[q % 2, :, cols] = prod[half:].astype(jnp.bfloat16)
            return 0

        lax.fori_loop(0, dtiles, tile, 0)
        pt_copy(q).start()

        @pl.when(q < 14)
        def _():
            h_load(q + 2).start()

    def far_terms():
        cut = d // 2

        def part(i):
            return pl.ds(i * cut, cut)

        def pt_part(q, i):
            return remote(
                other.at[q % 2, :, part(i)], slot(parts, q).at[:, part(i)],
                pt_send, pt_recv, q + 14 * i, partner,
            )

        def tile(n, _):
            for k in range(5):
                @pl.when(n == 2 * k)
                def _():
                    wd_copy(k).wait()

            block = w[span(n // 2, 1, ff), span(n % 2, 1, TILE)]
            prod = jnp.dot(hbuf[...], block, preferred_element_type=jnp.float32)
            cols = span(n, 1, TILE)
            for k in range(2):
                term[k, :, cols] = prod[2 * k * half : (2 * k + 1) * half]
                other[k, :, cols] = prod[(2 * k + 1) * half : 2 * (k + 1) * half].astype(jnp.bfloat16)
            return 0

        def pass_on(i):
            for q in (2, 3):
                pt_part(q, i).wait_recv()
                own = fetch(slot(parts, q).at[:, part(i)], pin.at[:, part(i)], 0)
                own.start()
                own.wait()
                to = slot(xbuf, (q - 2) * 2 + 1)
                add(q, to, 0, i * dtiles // 2, (i + 1) * dtiles // 2)
                remote(
                    to.at[:, part(i)], slot(sums, (q - 2) * 7 + 1).at[:, part(i)],
                    rs_send, rs_recv, (q - 2) * 7 + 1, ring[q - 2],
                ).start()

        for q in range(2):
            pt_copy(q).wait_send()
        lax.fori_loop(0, dtiles // 2, tile, 0)
        for q in (2, 3):
            pt_part(q, 0).start()
        lax.fori_loop(dtiles // 2, dtiles - 2, tile, 0)
        pass_on(0)
        lax.fori_loop(dtiles - 2, dtiles, tile, 0)
        for q in (2, 3):
            pt_part(q, 1).start()
            h_load(q + 2).start()
        pass_on(1)
        for i in range(2):
            for q in (2, 3):
                pt_part(q, i).wait_send()

    def send(q, way):
        m = q // 2
        pt_copy(q).wait_recv()
        own = fetch(slot(parts, q), pin, 0)
        own.start()
        before = m - 2 + m // 6

        rs_copy(before, way).wait_recv()
        rs_copy(m - 2, way).wait_send()
        got = fetch(slot(sums, way * 7 + before), rin.at[0], 1)
        got.start()
        got.wait()
        own.wait()
        add(q, slot(xbuf, way * 2 + m % 2), 1)
        rs_copy(m, way).start()

    def finish(q):
        way = q - 14
        h = 1 - way
        pt_copy(q).wait_recv()
        own = fetch(slot(parts, q), pin, 0)
        own.start()
        last = ((4, 6), (6, 4))[way]
        for k in range(2):
            rs_copy(last[k], k).wait_recv()
            fetch(slot(sums, k * 7 + last[k]), rin.at[k], 1 + k).start()
        for k in range(2):
            fetch(slot(sums, k * 7 + last[k]), rin.at[k], 1 + k).wait()
        own.wait()
        add(q, other.at[way], 2)
        pltpu.make_async_copy(other.at[way], out.at[pl.ds(h * half, half)], y_sem.at[way]).start()

    def step(q, _):
        down(q)
        for way in range(2):
            @pl.when((q > 4) & ((q - 1) % 2 == way))
            def _():
                send(q - 1, way)
        return 0

    far_terms()
    lax.fori_loop(4, 15, step, 0)
    down(15)

    def drain(m, _):
        for way in range(2):
            ag_copy(m, way).wait_send()
        return 0

    def drain_pair(i, _):
        for way in range(2):
            dd_copy(i, way).wait_send()
        return 0

    lax.fori_loop(0, 7, drain, 0)
    lax.fori_loop(0, 8, drain_pair, 0)
    pt_copy(14).wait_send()
    finish(14)
    pt_copy(15).wait_send()
    finish(15)
    for way in range(2):
        pltpu.make_async_copy(
            other.at[way], out.at[pl.ds((1 - way) * half, half)], y_sem.at[way]
        ).wait()
        for m in (5, 6):
            rs_copy(m, way).wait_send()


def solution(mesh):
    def step(x, w_gate, w_up, w_down):
        n, d = x.shape
        ff = w_gate.shape[1]
        half = n // 2
        bf = jnp.bfloat16
        hbm = pl.BlockSpec(memory_space=pl.ANY)
        dma = pltpu.SemaphoreType.DMA
        result = pl.pallas_call(
            _mlp_kernel,
            out_shape=[
                jax.ShapeDtypeStruct((n, d), bf),
                jax.ShapeDtypeStruct((16 * n, d), bf),
                jax.ShapeDtypeStruct((16 * n, ff), bf),
                jax.ShapeDtypeStruct((16 * half, d), bf),
                jax.ShapeDtypeStruct((14 * half, d), bf),
            ],
            in_specs=[hbm] * 4,
            out_specs=[hbm] * 5,
            scratch_shapes=[
                pltpu.VMEM((2 * d, ff), bf),
                pltpu.VMEM((4 * half, d), bf),
                pltpu.VMEM((5, ff, EARLY), bf),
                pltpu.VMEM((2 * n, ff), bf),
                pltpu.VMEM((2, half, d), jnp.float32),
                pltpu.VMEM((2, half, d), bf),
                pltpu.VMEM((half, d), bf),
                pltpu.VMEM((2, half, d), bf),
                dma((14,)), dma((14,)), dma((16,)), dma((16,)),
                dma((14,)), dma((14,)), dma((18,)), dma((18,)),
                dma((2, ff // TILE)), dma((2,)), dma((2,)), dma((5,)), dma((5,)), dma((3,)), dma((2,)),
            ],
            compiler_params=pltpu.CompilerParams(
                collective_id=0, has_side_effects=True, vmem_limit_bytes=67043328
            ),
        )(x, w_gate, w_up, w_down)
        return result[0]

    return jax.shard_map(
        step,
        mesh=mesh,
        in_specs=(P(("dp", "tp"), None), P(None, "tp"), P(None, "tp"), P("tp", None)),
        out_specs=P(("dp", "tp"), None),
        check_vma=False,
    )
```

```python
import jax
import jax.numpy as jnp
from jax import lax
from jax.experimental import pallas as pl
from jax.experimental.pallas import tpu as pltpu
from jax.sharding import PartitionSpec as P

MESH = pl.DeviceIdType.MESH
TILE = 512
EARLY = 256
POLL_AT = 5
SEND_AT = 3


def _device(r, c):
    y = r // 4
    z = r + y * (7 - 2 * r)
    return (y * 4 + z) * 2 + c


def _mlp_kernel(
    x, wg_hbm, wu_hbm, wd_hbm,
    out, xg, hid, parts, sums,
    w, xbuf, wd, hbuf, term, other, pin, rin,
    ag_send, ag_recv, dd_send, dd_recv, rs_send, rs_recv, pt_send, pt_recv,
    w_sem, x_sem, h_sem, wd_sem, early_sem, in_sem, y_sem,
):
    half = x.shape[0] // 2
    n_rows = 2 * half
    d, ff = wg_hbm.shape
    ftiles = ff // TILE
    dtiles = d // TILE
    wide = ff // 2
    t = lax.axis_index("tp")
    c = t % 2
    z = (t // 2) % 4
    y = t // 8
    r = z + y * (7 - 2 * z)
    right = _device((r + 1) % 8, c)
    left = _device((r + 7) % 8, c)
    partner = t + 1 - 2 * c
    ring = (right, left)

    def span(i, n, size):
        return pl.ds(pl.multiple_of(i * size, size), n * size)

    def rows(j, h, rel, n=1):
        return span((j * 2 + h) * 2 + rel, n, half)

    def remote(src, dst, s, q, i, dev):
        return pltpu.make_async_remote_copy(
            src_ref=src, dst_ref=dst, send_sem=s.at[i], recv_sem=q.at[i],
            device_id={"tp": dev}, device_id_type=MESH,
        )

    def gathered(i, way):
        if way == 0:
            return (i + 1) // 2, (i + 1) % 2
        return (8 - (i + 1) // 2) % 8, 1 - (i + 1) % 2

    def ag_copy(m, way, own=False):
        h = m % 2 if way == 0 else 1 - m % 2
        j = gathered(m + 1, way)[0]
        src_j = m // 2 if way == 0 else (8 - m // 2) % 8
        src = x.at[pl.ds(h * half, half)] if own else xg.at[rows(src_j, h, 0)]
        return remote(src, xg.at[rows(j, h, 0)], ag_send, ag_recv, way * 7 + m, ring[way])

    def dd_copy(i, way, own=False):
        j, h = gathered(i, way)
        src = x.at[pl.ds(h * half, half)] if own else xg.at[rows(j, h, 0)]
        return remote(src, xg.at[rows(j, h, 1)], dd_send, dd_recv, way * 8 + i, partner)

    def w_copy(k, n):
        cols = span(n, 1, TILE)
        return pltpu.make_async_copy(
            (wg_hbm, wu_hbm)[k].at[:, cols], w.at[pl.ds(k * d, d), cols], w_sem.at[k, n]
        )

    def x_load(i, way):
        j, h = gathered(i, way)
        return pltpu.make_async_copy(
            xg.at[rows(j, h, 0, 2)], xbuf.at[pl.ds(way * n_rows, n_rows)], x_sem.at[way]
        )

    def h_store(i, way):
        j, h = gathered(i, way)
        return pltpu.make_async_copy(
            hbuf.at[pl.ds(way * n_rows, n_rows)], hid.at[rows(j, h, 0, 2)], h_sem.at[way]
        )

    def slot(ref, i):
        return ref.at[span(i, 1, half)]

    def pt_copy(q):
        return remote(other.at[q % 2], slot(parts, q), pt_send, pt_recv, q, partner)

    def rs_copy(m, way, first=False):
        i = way * 7 + m
        src = rin.at[way] if first else slot(xbuf, way * 2 + m % 2)
        return remote(src, slot(sums, i), rs_send, rs_recv, i, ring[way])

    def fetch(src, dst, i):
        return pltpu.make_async_copy(src, dst, in_sem.at[i])

    def add(q, to, sources, first=0, last=dtiles):
        def tile(n, _):
            cols = span(n, 1, TILE)
            total = term[q % 2, :, cols] + pin[:, cols].astype(jnp.float32)
            for s in range(sources):
                total += rin[s, :, cols].astype(jnp.float32)
            to[:, cols] = total.astype(jnp.bfloat16)
            return 0

        lax.fori_loop(first, last, tile, 0)

    def early_copy(n):
        return pltpu.make_async_copy(
            wd_hbm.at[:, span(n, 1, EARLY)], wd.at[n % 5], early_sem.at[n % 5]
        )

    def early_terms():
        def tile(n, _):
            early_copy(n).wait()

            @pl.when(n == d // EARLY - 4)
            def _():
                ready(6)

            @pl.when(n + 4 < d // EARLY)
            def _():
                early_copy(n + 4).start()

            cols = span(n, 1, EARLY)
            prod = jnp.dot(hbuf[...], wd[n % 5], preferred_element_type=jnp.float32)
            term[1, :, cols] = prod[:half]
            other[1, :, cols] = prod[half:n_rows].astype(jnp.bfloat16)
            term[0, :, cols] = prod[n_rows : n_rows + half]
            other[0, :, cols] = prod[n_rows + half :].astype(jnp.bfloat16)
            return 0

        lax.fori_loop(0, d // EARLY, tile, 0)
        for q in range(2):
            pt_copy(q).start()

    def early_send():
        for q in range(2):
            pt_copy(q).wait_recv()
            own = fetch(slot(parts, q), pin, 0)
            own.start()
            own.wait()
            add(q, rin.at[q], 0)
            rs_copy(0, q, first=True).start()

    barrier = pltpu.get_barrier_semaphore()
    for dev in (right, left, partner):
        pl.semaphore_signal(barrier, inc=1, device_id={"tp": dev}, device_id_type=MESH)
    pl.semaphore_wait(barrier, 3)

    for way in range(2):
        dd_copy(0, way, own=True).start()
    for m in range(2):
        for way in range(2):
            ag_copy(m, way, own=True).start()
    mine = [
        pltpu.make_async_copy(
            x.at[pl.ds((1 - way) * half, half)], xbuf.at[pl.ds(2 * way * half, half)], x_sem.at[way]
        )
        for way in range(2)
    ]
    theirs = [
        pltpu.make_async_copy(
            xg.at[rows(0, 1 - way, 1)], xbuf.at[pl.ds((2 * way + 1) * half, half)], h_sem.at[way]
        )
        for way in range(2)
    ]
    for way in range(2):
        mine[way].start()
    for n in range(ftiles):
        for k in range(2):
            w_copy(k, n).start()
    for way in range(2):
        dd_copy(0, way, own=True).wait_recv()
        theirs[way].start()
    for way in range(2):
        mine[way].wait()
        theirs[way].wait()

    def poll(m):
        for k in range(2):
            ag_copy(m, k).wait_recv()
            dd_copy(m + 1, k).start()

            @pl.when(m < 5)
            def _():
                ag_copy(m + 2, k).start()

    def ready(i):
        for k in range(2):
            dd_copy(i, k).wait_recv()
        x_load(i, 0).start()

    def stage(i, _):
        def work(s, _):
            way, n = (s // 2) % 2, s // 4 * 2 + s % 2

            for k in range(2):
                @pl.when(s == 2 * k)
                def _():
                    @pl.when(i > 0)
                    def _():
                        if k == 0:
                            x_load(i, 1).start()
                        x_load(i, k).wait()
                        h_store(i - 1, k).wait()

            @pl.when((s == SEND_AT) & (i == 6))
            def _():
                early_send()

            @pl.when((s == 4) & (i == 7))
            def _():
                for k in range(5):
                    wd_copy(k).start()

            @pl.when((s == 4) & (i == 5))
            def _():
                for k in range(4):
                    early_copy(k).start()

            @pl.when((s == 6) & (i < 7))
            def _():
                h_store(i, 0).start()

            @pl.when((s == POLL_AT) & (i < 7) & (i != 5))
            def _():
                poll(i)

            @pl.when((s == 7) & (i < 7) & (i != 5))
            def _():
                ready(i + 1)

            for k in range(2):
                @pl.when((i == 0) & (way == 0))
                def _():
                    w_copy(k, n).wait()

            cols = span(n, 1, TILE)
            block = xbuf[span(way, 1, n_rows), :]
            gate = jnp.dot(block, w[:d, cols], preferred_element_type=jnp.float32)
            up = jnp.dot(block, w[d:, cols], preferred_element_type=jnp.float32)
            hbuf[span(way, 1, n_rows), cols] = (jax.nn.silu(gate) * up).astype(jnp.bfloat16)
            return 0

        lax.fori_loop(0, 2 * ftiles, work, 0)

        @pl.when(i < 7)
        def _():
            h_store(i, 1).start()

        @pl.when(i == 5)
        def _():
            poll(5)
            early_terms()

        return 0

    def wd_copy(k):
        return pltpu.make_async_copy(
            wd_hbm.at[:, pl.ds(k * wide, wide)],
            w.at[pl.ds(k * ff, ff), pl.ds(0, wide)],
            wd_sem.at[k],
        )

    lax.fori_loop(0, 8, stage, 0)

    def target(q):
        m, way = q // 2, q % 2
        j = 4 + m // 2 + (1 - m % 2) - m // 6 + 2 * (m // 7)
        h = (1 - m % 2) * (1 - m // 6) + m // 7
        sign = 1 - 2 * way
        return (8 + sign * j) % 8, way + sign * h

    def h_load(q):
        j, h = target(q)
        return pltpu.make_async_copy(
            hid.at[rows(j, h, 0, 2)], hbuf.at[span(q % 2, 1, n_rows)], h_sem.at[q % 2]
        )

    def down(q):
        h_load(q).wait()

        @pl.when(q >= 6)
        def _():
            pt_copy(q - 2).wait_send()

        def tile(n, _):
            block = w[span(n // 2, 1, ff), span(n % 2, 1, TILE)]
            prod = jnp.dot(
                hbuf[span(q % 2, 1, n_rows), :], block, preferred_element_type=jnp.float32
            )
            cols = span(n, 1, TILE)
            term[q % 2, :, cols] = prod[:half]
            other[q % 2, :, cols] = prod[half:].astype(jnp.bfloat16)
            return 0

        lax.fori_loop(0, dtiles, tile, 0)
        pt_copy(q).start()

        @pl.when(q < 14)
        def _():
            h_load(q + 2).start()

    def far_terms():
        cut = d // 2

        def part(i):
            return pl.ds(i * cut, cut)

        def pt_part(q, i):
            return remote(
                other.at[q % 2, :, part(i)], slot(parts, q).at[:, part(i)],
                pt_send, pt_recv, q + 14 * i, partner,
            )

        def tile(n, _):
            for k in range(5):
                @pl.when(n == 2 * k)
                def _():
                    wd_copy(k).wait()

            block = w[span(n // 2, 1, ff), span(n % 2, 1, TILE)]
            prod = jnp.dot(hbuf[...], block, preferred_element_type=jnp.float32)
            cols = span(n, 1, TILE)
            for k in range(2):
                term[k, :, cols] = prod[2 * k * half : (2 * k + 1) * half]
                other[k, :, cols] = prod[(2 * k + 1) * half : 2 * (k + 1) * half].astype(jnp.bfloat16)
            return 0

        def pass_on(i):
            for q in (2, 3):
                pt_part(q, i).wait_recv()
                own = fetch(slot(parts, q).at[:, part(i)], pin.at[:, part(i)], 0)
                own.start()
                own.wait()
                to = slot(xbuf, (q - 2) * 2 + 1)
                add(q, to, 0, i * dtiles // 2, (i + 1) * dtiles // 2)
                remote(
                    to.at[:, part(i)], slot(sums, (q - 2) * 7 + 1).at[:, part(i)],
                    rs_send, rs_recv, (q - 2) * 7 + 1, ring[q - 2],
                ).start()

        for q in range(2):
            pt_copy(q).wait_send()
        lax.fori_loop(0, dtiles // 2, tile, 0)
        for q in (2, 3):
            pt_part(q, 0).start()
        lax.fori_loop(dtiles // 2, dtiles - 2, tile, 0)
        pass_on(0)
        lax.fori_loop(dtiles - 2, dtiles, tile, 0)
        for q in (2, 3):
            pt_part(q, 1).start()
            h_load(q + 2).start()
        pass_on(1)
        for i in range(2):
            for q in (2, 3):
                pt_part(q, i).wait_send()

    def send(q, way):
        m = q // 2
        pt_copy(q).wait_recv()
        own = fetch(slot(parts, q), pin, 0)
        own.start()
        before = m - 2 + m // 6

        rs_copy(before, way).wait_recv()
        rs_copy(m - 2, way).wait_send()
        got = fetch(slot(sums, way * 7 + before), rin.at[0], 1)
        got.start()
        got.wait()
        own.wait()
        add(q, slot(xbuf, way * 2 + m % 2), 1)
        rs_copy(m, way).start()

    def fold(q, kept):
        way = q % 2
        pt_copy(q).wait_recv()
        loads = [fetch(slot(parts, q), pin, 0)]
        if kept is not None:
            rs_copy(kept, way).wait_recv()
            loads.append(fetch(slot(sums, way * 7 + kept), rin.at[0], 1))
        for load in loads:
            load.start()
        for load in loads:
            load.wait()

        def tile(n, _):
            cols = span(n, 1, TILE)
            total = term[q % 2, :, cols] + pin[:, cols].astype(jnp.float32)
            if kept is not None:
                total += rin[0, :, cols].astype(jnp.float32)
            term[q % 2, :, cols] = total
            return 0

        lax.fori_loop(0, dtiles, tile, 0)

    def last_add(k, src, to, i):
        def tile(n, _):
            cols = span(n, 1, TILE)
            to[:, cols] = (term[k, :, cols] + rin[src, :, cols].astype(jnp.float32)).astype(jnp.bfloat16)
            return 0

        lax.fori_loop(i * dtiles // 2, (i + 1) * dtiles // 2, tile, 0)

    def arrive(m):
        for way in range(2):
            rs_copy(m, way).wait_recv()
            fetch(slot(sums, way * 7 + m), rin.at[way], 1 + way).start()
        for way in range(2):
            fetch(slot(sums, way * 7 + m), rin.at[way], 1 + way).wait()

    def columns(i):
        return pl.ds(i * (d // 2), d // 2)

    def message(m, _):
        for way in range(2):
            down(2 * m + way)
        for way in range(2):
            send(2 * m + way, way)
        return 0

    far_terms()
    lax.fori_loop(2, 6, message, 0)

    for way in range(2):
        down(12 + way)
    for way in range(2):
        fold(12 + way, None)
        rs_copy(4, way).wait_send()
    arrive(5)
    for i in range(2):
        for way in range(2):
            to = slot(xbuf, way * 2)
            last_add(way, way, to, i)
            remote(
                to.at[:, columns(i)], slot(sums, way * 7 + 6).at[:, columns(i)],
                rs_send, rs_recv, way * 7 + 6, ring[way],
            ).start()

    def drain(m, _):
        for way in range(2):
            ag_copy(m, way).wait_send()
        return 0

    def drain_pair(i, _):
        for way in range(2):
            dd_copy(i, way).wait_send()
        return 0

    for way in range(2):
        down(14 + way)
    lax.fori_loop(0, 7, drain, 0)
    lax.fori_loop(0, 8, drain_pair, 0)
    for way in range(2):
        fold(14 + way, 4)
        pt_copy(14 + way).wait_send()
        rs_copy(5, way).wait_send()
    arrive(6)

    def result(k, i):
        return pltpu.make_async_copy(
            other.at[k, :, columns(i)], out.at[pl.ds((1 - k) * half, half), columns(i)], y_sem.at[k, i]
        )

    for i in range(2):
        for k in range(2):
            last_add(k, 1 - k, other.at[k], i)
            result(k, i).start()
    for i in range(2):
        for k in range(2):
            result(k, i).wait()
    for way in range(2):
        rs_copy(6, way).wait_send()


def solution(mesh):
    def step(x, w_gate, w_up, w_down):
        n, d = x.shape
        ff = w_gate.shape[1]
        half = n // 2
        bf = jnp.bfloat16
        hbm = pl.BlockSpec(memory_space=pl.ANY)
        dma = pltpu.SemaphoreType.DMA
        result = pl.pallas_call(
            _mlp_kernel,
            out_shape=[
                jax.ShapeDtypeStruct((n, d), bf),
                jax.ShapeDtypeStruct((16 * n, d), bf),
                jax.ShapeDtypeStruct((16 * n, ff), bf),
                jax.ShapeDtypeStruct((16 * half, d), bf),
                jax.ShapeDtypeStruct((14 * half, d), bf),
            ],
            in_specs=[hbm] * 4,
            out_specs=[hbm] * 5,
            scratch_shapes=[
                pltpu.VMEM((2 * d, ff), bf),
                pltpu.VMEM((4 * half, d), bf),
                pltpu.VMEM((5, ff, EARLY), bf),
                pltpu.VMEM((2 * n, ff), bf),
                pltpu.VMEM((2, half, d), jnp.float32),
                pltpu.VMEM((2, half, d), bf),
                pltpu.VMEM((half, d), bf),
                pltpu.VMEM((2, half, d), bf),
                dma((14,)), dma((14,)), dma((16,)), dma((16,)),
                dma((14,)), dma((14,)), dma((18,)), dma((18,)),
                dma((2, ff // TILE)), dma((2,)), dma((2,)), dma((5,)), dma((5,)), dma((3,)), dma((2, 2)),
            ],
            compiler_params=pltpu.CompilerParams(
                collective_id=0, has_side_effects=True, vmem_limit_bytes=67043328
            ),
        )(x, w_gate, w_up, w_down)
        return result[0]

    return jax.shard_map(
        step,
        mesh=mesh,
        in_specs=(P(("dp", "tp"), None), P(None, "tp"), P(None, "tp"), P("tp", None)),
        out_specs=P(("dp", "tp"), None),
        check_vma=False,
    )
```
